32 devices in a mesh: clump: 8 (over z, y), grp: 4 (over x, core).
Axes of the slice: x: 2, y: 2, z: 4, core: 2. Of those that a mesh axis runs over, the one named last changes fastest.
Arguments:
- flux: float32 [32, 1024, 64], P(('clump', 'grp')), may hold values from -6 to 6
- patch_pft: int32 [32, 1024], P(('clump', 'grp')), may hold values from 0 to 15
- patch_wt: float32 [32, 1024], P(('clump', 'grp')), may hold values from 0.2 to 2
- patch_col: int32 [32, 1024], P(('clump', 'grp')), may hold values from 0 to 511, never falling along the last dimension, each value on 1 to 4 neighbouring positions
- col_wt: float32 [32, 512], P(('clump', 'grp')), may hold values from 0.2 to 2
- col_lu: int32 [32, 512], P(('clump', 'grp')), may hold values from 0 to 255, never falling along the last dimension, each value on 1 to 4 neighbouring positions
- lu_wt: float32 [32, 256], P(('clump', 'grp')), may hold values from 0.2 to 2
- lu_grid: int32 [32, 256], P(('clump', 'grp')), may hold values from 0 to 127, never falling along the last dimension, each value on 1 to 4 neighbouring positions
- cell_target: int32 [32, 128], P(('clump', 'grp')), may hold values from 0 to 4095, as said below
- patch_count: int32 [32], P(('clump', 'grp')), may hold values from 64 to 1024
- pft_scale: float32 [16, 64], replicated, may hold values from 0.3 to 3
- cpl_frac: float32 [4096], P(('clump', 'grp')), may hold values from 0.2 to 0.9
- cpl_field: float32 [4096, 64], P(('clump', 'grp')), may hold values from -6 to 6
Outputs:
- grid_merged: float32 [4096, 64], P(('clump', 'grp'))
- anomaly: float32 [32, 1024, 64], P(('clump', 'grp'))
The draws below stay inside these ranges and needn't reach their ends.
Inputs may be any that keep to these rules, and one draw needn't show every extreme that they name: `patch_col`: within each device's row the column numbers never fall, and each column holds 1 to 4 patch slots. `col_lu`: within each device's row the landunit numbers never fall, and each landunit holds 1 to 4 columns. `lu_grid`: within each device's row the gridcell numbers never fall, and each gridcell holds 1 to 4 landunits. `cell_target`: all devices' entries together are a permutation of 0 to 4095; the coupler owner of an entry q is q // 128, and each device's 128 gridcells go to 16 owners, exactly 8 to each.
All inputs are finite; a program needn't handle non-finite values.
Results may differ from the reference program's by a relative error of at most 0.0003.
Values sent between devices are 32-bit elements; how exact they have to be, the bound alone decides.
No kernel may reach another device: no remote copies, remote signals or barrier semaphores. Data moves between devices by JAX's collectives and lax.ppermute only.
A program may use at most 64 MiB of HBM per device.

```python
import math
import jax
import jax.numpy as jnp
import numpy as np
from jax import lax

NV = 64
NPFT = 16
P_DEV = 1024
C_DEV = 512
L_DEV = 256
G_DEV = 128
CAP = 8
GRID = 4096
DEVICES = 32


def row_orders(key, rows, length):

    def single(row_key):
        return jax.random.permutation(row_key, length)
    return jax.vmap(single)(jax.random.split(key, rows))


def draw_cell_target(key, part):
    key_shift, key_label, key_local, key_slot = jax.random.split(jax.random.fold_in(key, 11), 4)
    shift = jax.random.permutation(key_shift, DEVICES).astype(jnp.int32)
    label = jax.random.permutation(key_label, DEVICES).astype(jnp.int32)
    local_order = row_orders(key_local, DEVICES, G_DEV).astype(jnp.int32)
    slot_order = row_orders(key_slot, DEVICES, G_DEV).astype(jnp.int32)
    block_of = local_order // CAP
    pre_owner = (block_of + shift[:, None]) % DEVICES
    owner_dev = label[pre_owner]
    slot_in = slot_order[pre_owner, local_order]
    return (owner_dev * G_DEV + slot_in).astype(jnp.int32)


def place_ends(result, key, least, largest):
    index_at = [jax.random.randint(jax.random.fold_in(key, axis), (), 0, length) for axis, length in enumerate(result.shape)]
    widest = result.shape.index(max(result.shape))
    beside = index_at[:widest] + [(index_at[widest] + 1) % result.shape[widest]] + index_at[widest + 1:]
    return result.at[tuple(index_at)].set(least).at[tuple(beside)].set(largest)


def steps_of(key, dims, cuts, smallest, high):
    factor_of = 1.0
    for dim, parts in cuts:
        steps = jax.random.uniform(jax.random.fold_in(jax.random.fold_in(key, 6), dim), (parts,), jnp.float32, smallest / len(cuts), high / len(cuts))
        factor_of = factor_of * jnp.repeat(jnp.exp(steps), dims[dim] // parts).reshape((-1,) + (1,) * (len(dims) - 1 - dim))
    return factor_of


def split_up(count, total, most, lean):
    loads = [(1 << 20) // math.isqrt(standing ** lean) + 1 for standing in range(2, count + 1)]
    spare, counts = total - most - (count - 1), [1] * (count - 1)
    while spare > 0:
        candidates = [i for i in range(count - 1) if counts[i] < most]
        mass, left = sum([loads[i] for i in candidates]), spare
        for i in candidates:
            more = min(most - counts[i], max(1, left * loads[i] // mass), spare)
            counts[i] = counts[i] + more
            spare = spare - more
    return np.array([most] + counts)


def ragged(own_key, number_of, total, most, slope):
    if number_of == 2:
        one = jax.random.randint(own_key, (), max(1, total - most), min(most, total - 1) + 1)
        return jnp.stack([one, total - one])
    tallies = jnp.asarray(split_up(number_of, total, most, slope), jnp.int32)
    couples = (number_of - 1) // 2
    giver, sink = tallies[1:1 + 2 * couples:2], tallies[2:2 + 2 * couples:2]
    margin = jnp.minimum(giver - 1, most - sink)
    passed = jax.random.randint(jax.random.fold_in(own_key, 1), (couples,), 0, 1 << 20) % (margin + 1)
    tallies = tallies.at[1:1 + 2 * couples:2].set(giver - passed).at[2:2 + 2 * couples:2].set(sink + passed)
    return tallies[jax.random.permutation(jax.random.fold_in(own_key, 2), number_of)]


def gaussian(rng, dims, deviation, reach, pieces=(), kind=jnp.bfloat16):
    factor_of = steps_of(rng, dims, pieces, -0.22, 0.18) if pieces else 1.0
    array = jax.random.normal(rng, dims, jnp.float32) * deviation * factor_of
    return jnp.minimum(jnp.maximum(array, -reach), reach).astype(kind)


def setup_inputs(seed: int = 0) -> dict:
    seeds = jax.random.split(jax.random.key(seed), 14)
    flux = gaussian(seeds[0], (DEVICES, P_DEV, NV), 1.0, 6.0, ((0, 32),), jnp.float32)
    patch_pft = place_ends(jax.random.randint(seeds[1], (DEVICES, P_DEV), 0, NPFT), jax.random.fold_in(seeds[1], 1), 0, NPFT - 1).astype(jnp.int32)
    patch_wt = jnp.clip(jnp.exp(math.log(2.0) - 2.3025851 * jax.random.uniform(seeds[2], (DEVICES, P_DEV), jnp.float32) ** steps_of(seeds[2], (DEVICES, P_DEV), ((0, 32),), -0.2, 0.2)), 0.2, 2.0)
    patch_col = jax.vmap(lambda own: jnp.searchsorted(jnp.cumsum(ragged(own, C_DEV, P_DEV, 4, 1)), jnp.arange(P_DEV), side="right"))(jax.random.split(seeds[3], DEVICES)).reshape((DEVICES, P_DEV)).astype(jnp.int32)
    col_wt = jnp.clip(jnp.exp(math.log(2.0) - 2.3025851 * jax.random.uniform(seeds[4], (DEVICES, C_DEV), jnp.float32) ** steps_of(seeds[4], (DEVICES, C_DEV), ((0, 32),), -0.2, 0.2)), 0.2, 2.0)
    col_lu = jax.vmap(lambda own: jnp.searchsorted(jnp.cumsum(ragged(own, L_DEV, C_DEV, 4, 1)), jnp.arange(C_DEV), side="right"))(jax.random.split(seeds[5], DEVICES)).reshape((DEVICES, C_DEV)).astype(jnp.int32)
    lu_wt = jnp.clip(jnp.exp(math.log(2.0) - 2.3025851 * jax.random.uniform(seeds[6], (DEVICES, L_DEV), jnp.float32) ** steps_of(seeds[6], (DEVICES, L_DEV), ((0, 32),), -0.2, 0.2)), 0.2, 2.0)
    lu_grid = jax.vmap(lambda own: jnp.searchsorted(jnp.cumsum(ragged(own, G_DEV, L_DEV, 4, 1)), jnp.arange(L_DEV), side="right"))(jax.random.split(seeds[7], DEVICES)).reshape((DEVICES, L_DEV)).astype(jnp.int32)
    cell_target = draw_cell_target(jax.random.fold_in(seeds[13], 71), 0)
    patch_count = place_ends(jax.random.randint(seeds[9], (DEVICES,), P_DEV // 16, P_DEV + 1), jax.random.fold_in(seeds[9], 1), P_DEV // 16, P_DEV).astype(jnp.int32)
    pft_scale = jnp.clip(jnp.exp(jax.random.uniform(seeds[10], (NPFT, NV), jnp.float32, math.log(0.3), math.log(3.0))), 0.3, 3.0)
    cpl_frac = jnp.clip(0.2 + 0.7 * jax.random.uniform(seeds[11], (GRID,), jnp.float32) ** steps_of(seeds[11], (GRID,), ((0, 32),), -0.2, 0.2), 0.2, 0.9)
    cpl_field = gaussian(seeds[12], (GRID, NV), 1.0, 6.0, ((0, 32),), jnp.float32)
    return {"flux": flux, "patch_pft": patch_pft, "patch_wt": patch_wt, "patch_col": patch_col, "col_wt": col_wt, "col_lu": col_lu, "lu_wt": lu_wt, "lu_grid": lu_grid, "cell_target": cell_target, "patch_count": patch_count, "pft_scale": pft_scale, "cpl_frac": cpl_frac, "cpl_field": cpl_field}


def reference(flux, patch_pft, patch_wt, patch_col, col_wt, col_lu, lu_wt, lu_grid, cell_target, patch_count, pft_scale, cpl_frac, cpl_field):
    position = jnp.arange(P_DEV, dtype=jnp.int32)

    def local_means(entries):
        values, pft_ids, pweight, columns, cweight, colland, lweight, lugrid, live_count = entries
        alive_mask = (position < live_count).astype(jnp.float32)
        scaled = values * pft_scale[pft_ids]
        land_of = colland[columns]
        home_of = lugrid[land_of]
        weight_eff = alive_mask * pweight * cweight[columns] * lweight[land_of]
        numer = jax.ops.segment_sum(scaled * weight_eff[:, None], home_of, G_DEV)
        denom = jax.ops.segment_sum(weight_eff, home_of, G_DEV)
        return numer / jnp.maximum(denom, 1.0)[:, None]

    cell_mean = lax.map(local_means, (flux, patch_pft, patch_wt, patch_col, col_wt, col_lu, lu_wt, lu_grid, patch_count))
    placed = jnp.zeros((GRID, NV), jnp.float32).at[cell_target.reshape(-1)].set(cell_mean.reshape(-1, NV))
    grid_merged = cpl_frac[:, None] * placed + (1.0 - cpl_frac)[:, None] * cpl_field

    def local_anomaly(entries):
        values, pft_ids, columns, colland, lugrid, targets, live_count = entries
        alive_mask = (position < live_count).astype(jnp.float32)
        scaled = values * pft_scale[pft_ids]
        home_of = lugrid[colland[columns]]
        cell_merged = grid_merged[targets]
        return alive_mask[:, None] * (scaled - cell_merged[home_of])

    anomaly = lax.map(local_anomaly, (flux, patch_pft, patch_col, col_lu, lu_grid, cell_target, patch_count))
    return grid_merged, anomaly
```

```python
import functools

import jax
import jax.numpy as jnp
from jax import lax
from jax.experimental import pallas as pl
from jax.experimental.pallas import tpu as pltpu
from jax.sharding import PartitionSpec as P

AXES = ("clump", "grp")
LANES = 128
F32, BF16, I32 = jnp.float32, jnp.bfloat16, jnp.int32


def iota(shape, dim):
    return lax.broadcasted_iota(I32, shape, dim)


def split(x):
    high = x.astype(BF16)
    return high, (x - high.astype(F32)).astype(BF16)


def onehot(mask):
    return jnp.where(mask, 1.0, 0.0).astype(BF16)


def dot_nn(a, b):
    return lax.dot_general(a, b, (((1,), (0,)), ((), ())), preferred_element_type=F32)


def dot_nt(a, b):
    return lax.dot_general(a, b, (((1,), (1,)), ((), ())), preferred_element_type=F32)


def lookup(table, index):
    shape = index.shape
    lane, row = index & (LANES - 1), index >> 7
    out = None
    for r in range(table.shape[0]):
        line = jnp.broadcast_to(table[r : r + 1, :], shape)
        got = jnp.take_along_axis(line, lane, axis=1, mode="promise_in_bounds")
        out = got if out is None else jnp.where(row == r, got, out)
    return out


def as_row(x):
    return jnp.concatenate([x[s : s + 1, :] for s in range(x.shape[0])], axis=1)


def ranks(mask):
    before = onehot(iota((LANES, LANES), 0) < iota((LANES, LANES), 1))
    return dot_nn(onehot(mask), before)


def local_kernel(
    n_dev, count, flux, pft, pwt, pcol, cwt, clu, lwt, lgrid, target, scale, kept, mean, home_out, slot_out
):
    nv, patches = flux.shape
    cells = target.shape[1]
    index = pcol[...]
    land = lookup(clu[...], index)
    home = lookup(lgrid[...], land)
    weight = pwt[...] * lookup(cwt[...], index) * lookup(lwt[...], land)
    position = iota(index.shape, 0) * LANES + iota(index.shape, 1)
    alive = position < count[0]
    home = jnp.where(alive, home, -1)
    weight = jnp.where(alive, weight, 0.0)
    home_out[...] = home
    types = scale.shape[0]
    type_hot = onehot(iota((types, patches), 0) == as_row(pft[...]))
    scale_t = jnp.concatenate(split(scale[...]), axis=1).T
    factor = dot_nn(scale_t, type_hot)
    home_row = as_row(home)
    scaled = jnp.where(home_row >= 0, flux[...] * (factor[:nv] + factor[nv:]), 0.0)
    kept[...] = scaled
    weight_row = as_row(weight)
    high, low = split(scaled * weight_row)
    w_high, w_low = split(jnp.broadcast_to(weight_row, (16, patches)))
    w_both = jnp.where(iota((16, patches), 0) == 0, w_high, w_low)
    home_hot = onehot(iota((cells, patches), 0) == home_row)
    sums = dot_nt(jnp.concatenate([high, low, w_both], axis=0), home_hot)
    den = sums[2 * nv : 2 * nv + 1] + sums[2 * nv + 1 : 2 * nv + 2]
    mean[...] = (sums[:nv] + sums[nv : 2 * nv]) / jnp.maximum(den, 1.0)
    owner = target[...] // cells
    owned = iota((n_dev, cells), 0) == owner
    rank = jnp.sum(jnp.where(owned, ranks(owned), 0.0), axis=0, keepdims=True)
    slot_out[...] = rank.astype(I32) * n_dev + owner


def pack_kernel(n_dev, cap, me, heard, mean, slot, target, field, send, field_hot_out, frac_out):
    nv, cells = field.shape
    slots = n_dev * cap
    table = heard[pl.ds(0, n_dev, stride=2), :].astype(I32)
    owner = table // cells
    local = (table - owner * cells).astype(F32)
    mine = owner == me[0]
    rank = ranks(mine)
    asked = jnp.concatenate(
        [jnp.where(mine & (rank == r), local + 1.0, 0.0) for r in range(cap)], axis=0
    ).astype(BF16)
    wanted = dot_nn(asked, jnp.ones((cells, cells), BF16))
    lane = iota((slots, cells), 1)
    field_hot = onehot(wanted == (lane + 1).astype(F32))
    mean_hot = onehot(iota((slots, cells), 0) == slot[...])
    field_hot_out[...] = field_hot
    m_high, m_low = split(mean[...])
    f_high, f_low = split(field[...])
    zero = jnp.zeros((nv, 2 * cells), BF16)
    rows = jnp.concatenate(
        [
            jnp.concatenate([m_high, m_low, zero], axis=1),
            jnp.concatenate([zero, f_high, f_low], axis=1),
        ],
        axis=0,
    )
    out = dot_nt(jnp.concatenate([mean_hot, mean_hot, field_hot, field_hot], axis=1), rows)
    for r in range(cap):
        send[pl.ds(r, n_dev, stride=cap), :] = out[r * n_dev : (r + 1) * n_dev, :]
    goal = target[...]
    goal_owner = goal // cells
    goal_local = jnp.broadcast_to(goal - goal_owner * cells, (n_dev, cells))
    fracs = heard[pl.ds(1, n_dev, stride=2), :]
    picked = jnp.take_along_axis(fracs, goal_local, axis=1, mode="promise_in_bounds")
    picked = jnp.where(iota((n_dev, cells), 0) == goal_owner, picked, 0.0)
    frac_out[...] = jnp.sum(picked, axis=0, keepdims=True)


def finish_kernel(
    n_dev, cap, got, field_hot, slot, frac, mean, kept, home, own_frac, field, merged_out, anomaly_out
):
    nv, cells = field.shape
    patches = kept.shape[1]
    slots = n_dev * cap
    rows = jnp.concatenate([got[pl.ds(r, n_dev, stride=cap), :] for r in range(cap)], axis=0)
    high, low = split(rows.T)
    mean_hot = onehot(iota((slots, cells), 0) == slot[...])
    hots = jnp.concatenate([field_hot[...], mean_hot], axis=1)
    both = dot_nn(jnp.concatenate([high, low], axis=0), hots)
    width = 2 * nv
    both = both[:width] + both[width:]
    own = own_frac[...]
    merged_out[...] = own * both[:nv, :cells] + (1.0 - own) * field[...]
    part = frac[...]
    merged = part * mean[...] + (1.0 - part) * both[nv:, cells:]
    home_hot = onehot(iota((cells, patches), 0) == as_row(home[...]))
    picked = dot_nn(jnp.concatenate(split(merged), axis=0), home_hot)
    anomaly_out[...] = kept[...] - (picked[:nv] + picked[nv:])


def shape(dims, dtype=F32):
    return jax.ShapeDtypeStruct(dims, dtype)


def call(body, outs, n_args, scalars, flops):
    vmem = pl.BlockSpec(memory_space=pltpu.VMEM)
    smem = pl.BlockSpec(memory_space=pltpu.SMEM)
    return pl.pallas_call(
        body,
        out_shape=outs,
        in_specs=[smem] * scalars + [vmem] * (n_args - scalars),
        out_specs=[vmem] * len(outs),
        cost_estimate=pl.CostEstimate(flops=flops, bytes_accessed=1 << 20, transcendentals=0),
    )


def per_device(
    flux,
    patch_pft,
    patch_wt,
    patch_col,
    col_wt,
    col_lu,
    lu_wt,
    lu_grid,
    cell_target,
    patch_count,
    pft_scale,
    cpl_frac,
    cpl_field,
):
    n_dev = lax.axis_size("clump") * lax.axis_size("grp")
    patches, nv = flux.shape[1:]
    cells = cell_target.shape[1]
    cap = max(2, 2 * cells // n_dev)
    slots = n_dev * cap
    lanes = lambda x: x.reshape(-1, LANES)
    exchange = lambda x: lax.all_to_all(x, AXES, split_axis=0, concat_axis=0, tiled=True)

    frac_row = cpl_frac.reshape(1, cells)
    told = jnp.concatenate([cell_target.astype(F32), frac_row], axis=0)
    told = jnp.broadcast_to(told[None], (n_dev, 2, cells)).reshape(2 * n_dev, cells)
    heard = exchange(told)

    field_t = cpl_field.T
    kept, mean, home, slot = call(
        functools.partial(local_kernel, n_dev),
        [
            shape((nv, patches)),
            shape((nv, cells)),
            shape((patches // LANES, LANES), I32),
            shape((1, cells), I32),
        ],
        11,
        1,
        1 << 28,
    )(
        patch_count,
        flux[0].T,
        lanes(patch_pft),
        lanes(patch_wt),
        lanes(patch_col),
        lanes(col_wt),
        lanes(col_lu),
        lanes(lu_wt),
        lanes(lu_grid),
        cell_target,
        pft_scale,
    )
    me = lax.axis_index(AXES).astype(I32).reshape(1)
    send, field_hot, frac = call(
        functools.partial(pack_kernel, n_dev, cap),
        [shape((slots, 2 * nv)), shape((slots, cells), BF16), shape((1, cells))],
        6,
        1,
        1 << 26,
    )(me, heard, mean, slot, cell_target, field_t)
    got = exchange(send)
    merged, anomaly = call(
        functools.partial(finish_kernel, n_dev, cap),
        [shape((nv, cells)), shape((nv, patches))],
        9,
        0,
        1 << 26,
    )(got, field_hot, slot, frac, mean, kept, home, frac_row, field_t)
    return merged.T, anomaly.T[None]


def solution(mesh):
    split_1 = P(AXES)
    split_2 = P(AXES, None)
    split_3 = P(AXES, None, None)
    return jax.shard_map(
        per_device,
        mesh=mesh,
        in_specs=(split_3,) + (split_2,) * 8 + (split_1, P(), split_1, split_2),
        out_specs=(split_2, split_3),
        check_vma=False,
    )
```

```python
import functools

import jax
import jax.numpy as jnp
from jax import lax
from jax.experimental import pallas as pl
from jax.experimental.pallas import tpu as pltpu
from jax.sharding import PartitionSpec as P

AXES = ("clump", "grp")
LANES = 128
F32, BF16, I32 = jnp.float32, jnp.bfloat16, jnp.int32


def iota(shape, dim):
    return lax.broadcasted_iota(I32, shape, dim)


def split(x):
    high = x.astype(BF16)
    return high, (x - high.astype(F32)).astype(BF16)


def onehot(mask):
    return jnp.where(mask, 1.0, 0.0).astype(BF16)


def dot_nn(a, b):
    return lax.dot_general(a, b, (((1,), (0,)), ((), ())), preferred_element_type=F32)


def dot_nt(a, b):
    return lax.dot_general(a, b, (((1,), (1,)), ((), ())), preferred_element_type=F32)


def lookup(table, index):
    shape = index.shape
    lane, row = index & (LANES - 1), index >> 7
    out = None
    for r in range(table.shape[0]):
        line = jnp.broadcast_to(table[r : r + 1, :], shape)
        got = jnp.take_along_axis(line, lane, axis=1, mode="promise_in_bounds")
        out = got if out is None else jnp.where(row == r, got, out)
    return out


def as_row(x):
    return jnp.concatenate([x[s : s + 1, :] for s in range(x.shape[0])], axis=1)


def ranks(mask):
    before = onehot(iota((LANES, LANES), 0) < iota((LANES, LANES), 1))
    return dot_nn(onehot(mask), before)


def local_kernel(
    n_dev, count, flux, pft, pwt, pcol, cwt, clu, lwt, lgrid, target, scale, kept, mean, home_out, slot_out
):
    nv, patches = flux.shape
    cells = target.shape[1]
    index = pcol[...]
    land = lookup(clu[...], index)
    home = lookup(lgrid[...], land)
    weight = pwt[...] * lookup(cwt[...], index) * lookup(lwt[...], land)
    position = iota(index.shape, 0) * LANES + iota(index.shape, 1)
    alive = position < count[0]
    home = jnp.where(alive, home, -1)
    weight = jnp.where(alive, weight, 0.0)
    home_out[...] = home
    types = scale.shape[0]
    type_hot = onehot(iota((types, patches), 0) == as_row(pft[...]))
    scale_t = jnp.concatenate(split(scale[...]), axis=1).T
    factor = dot_nn(scale_t, type_hot)
    home_row = as_row(home)
    scaled = jnp.where(home_row >= 0, flux[...] * (factor[:nv] + factor[nv:]), 0.0)
    kept[...] = scaled
    weight_row = as_row(weight)
    high, low = split(scaled * weight_row)
    w_high, w_low = split(jnp.broadcast_to(weight_row, (16, patches)))
    w_both = jnp.where(iota((16, patches), 0) == 0, w_high, w_low)
    home_hot = onehot(iota((cells, patches), 0) == home_row)
    sums = dot_nt(jnp.concatenate([high, low, w_both], axis=0), home_hot)
    den = sums[2 * nv : 2 * nv + 1] + sums[2 * nv + 1 : 2 * nv + 2]
    mean[...] = (sums[:nv] + sums[nv : 2 * nv]) / jnp.maximum(den, 1.0)
    owner = target[...] // cells
    owned = iota((n_dev, cells), 0) == owner
    rank = jnp.sum(jnp.where(owned, ranks(owned), 0.0), axis=0, keepdims=True)
    slot_out[...] = rank.astype(I32) * n_dev + owner


def pack_kernel(n_dev, cap, me, heard, mean, slot, target, field, send, field_hot_out, frac_out):
    nv, cells = field.shape
    slots = n_dev * cap
    table = heard[pl.ds(0, n_dev, stride=2), :].astype(I32)
    owner = table // cells
    local = (table - owner * cells).astype(F32)
    mine = owner == me[0]
    rank = ranks(mine)
    asked = jnp.concatenate(
        [jnp.where(mine & (rank == r), local + 1.0, 0.0) for r in range(cap)], axis=0
    ).astype(BF16)
    wanted = dot_nn(asked, jnp.ones((cells, cells), BF16))
    lane = iota((slots, cells), 1)
    field_hot = onehot(wanted == (lane + 1).astype(F32))
    mean_hot = onehot(iota((slots, cells), 0) == slot[...])
    field_hot_out[...] = field_hot
    m_high, m_low = split(mean[...])
    f_high, f_low = split(field[...])
    zero = jnp.zeros((nv, 2 * cells), BF16)
    rows = jnp.concatenate(
        [
            jnp.concatenate([m_high, m_low, zero], axis=1),
            jnp.concatenate([zero, f_high, f_low], axis=1),
        ],
        axis=0,
    )
    out = dot_nt(jnp.concatenate([mean_hot, mean_hot, field_hot, field_hot], axis=1), rows)
    for r in range(cap):
        send[pl.ds(r, n_dev, stride=cap), :] = out[r * n_dev : (r + 1) * n_dev, :]
    goal = target[...]
    goal_owner = goal // cells
    goal_local = jnp.broadcast_to(goal - goal_owner * cells, (n_dev, cells))
    fracs = heard[pl.ds(1, n_dev, stride=2), :]
    picked = jnp.take_along_axis(fracs, goal_local, axis=1, mode="promise_in_bounds")
    picked = jnp.where(iota((n_dev, cells), 0) == goal_owner, picked, 0.0)
    frac_out[...] = jnp.sum(picked, axis=0, keepdims=True)


def finish_kernel(
    n_dev, cap, got, field_hot, slot, frac, mean, kept, home, own_frac, field, merged_out, anomaly_out
):
    nv, cells = field.shape
    patches = kept.shape[1]
    slots = n_dev * cap
    rows = jnp.concatenate([got[pl.ds(r, n_dev, stride=cap), :] for r in range(cap)], axis=0)
    high, low = split(rows.T)
    mean_hot = onehot(iota((slots, cells), 0) == slot[...])
    hots = jnp.concatenate([field_hot[...], mean_hot], axis=1)
    both = dot_nn(jnp.concatenate([high, low], axis=0), hots)
    width = 2 * nv
    both = both[:width] + both[width:]
    own = own_frac[...]
    merged_out[...] = own * both[:nv, :cells] + (1.0 - own) * field[...]
    part = frac[...]
    merged = part * mean[...] + (1.0 - part) * both[nv:, cells:]
    home_hot = onehot(iota((cells, patches), 0) == as_row(home[...]))
    picked = dot_nn(jnp.concatenate(split(merged), axis=0), home_hot)
    anomaly_out[...] = kept[...] - (picked[:nv] + picked[nv:])


def shape(dims, dtype=F32):
    return jax.ShapeDtypeStruct(dims, dtype)


def call(body, outs, n_args, scalars, flops):
    vmem = pl.BlockSpec(memory_space=pltpu.VMEM)
    smem = pl.BlockSpec(memory_space=pltpu.SMEM)
    return pl.pallas_call(
        body,
        out_shape=outs,
        in_specs=[smem] * scalars + [vmem] * (n_args - scalars),
        out_specs=[vmem] * len(outs),
        compiler_params=pltpu.CompilerParams(vmem_limit_bytes=16 << 20),
        cost_estimate=pl.CostEstimate(flops=flops, bytes_accessed=1 << 20, transcendentals=0),
    )


def per_device(
    flux,
    patch_pft,
    patch_wt,
    patch_col,
    col_wt,
    col_lu,
    lu_wt,
    lu_grid,
    cell_target,
    patch_count,
    pft_scale,
    cpl_frac,
    cpl_field,
):
    n_dev = lax.axis_size("clump") * lax.axis_size("grp")
    patches, nv = flux.shape[1:]
    cells = cell_target.shape[1]
    cap = max(2, 2 * cells // n_dev)
    slots = n_dev * cap
    lanes = lambda x: x.reshape(-1, LANES)
    exchange = lambda x: lax.all_to_all(x, AXES, split_axis=0, concat_axis=0, tiled=True)

    frac_row = cpl_frac.reshape(1, cells)
    dims = (2 * n_dev, cells)
    goals = jnp.broadcast_to(cell_target.astype(F32), dims)
    heard = exchange(jnp.where(iota(dims, 0) % 2 == 0, goals, jnp.broadcast_to(frac_row, dims)))

    field_t = cpl_field.T
    kept, mean, home, slot = call(
        functools.partial(local_kernel, n_dev),
        [
            shape((nv, patches)),
            shape((nv, cells)),
            shape((patches // LANES, LANES), I32),
            shape((1, cells), I32),
        ],
        11,
        1,
        1 << 28,
    )(
        patch_count,
        flux[0].T,
        lanes(patch_pft),
        lanes(patch_wt),
        lanes(patch_col),
        lanes(col_wt),
        lanes(col_lu),
        lanes(lu_wt),
        lanes(lu_grid),
        cell_target,
        pft_scale,
    )
    me = lax.axis_index(AXES).astype(I32).reshape(1)
    send, field_hot, frac = call(
        functools.partial(pack_kernel, n_dev, cap),
        [shape((slots, 2 * nv)), shape((slots, cells), BF16), shape((1, cells))],
        6,
        1,
        1 << 26,
    )(me, heard, mean, slot, cell_target, field_t)
    got = exchange(send)
    merged, anomaly = call(
        functools.partial(finish_kernel, n_dev, cap),
        [shape((nv, cells)), shape((nv, patches))],
        9,
        0,
        1 << 26,
    )(got, field_hot, slot, frac, mean, kept, home, frac_row, field_t)
    return merged.T, anomaly.T[None]


def solution(mesh):
    split_1 = P(AXES)
    split_2 = P(AXES, None)
    split_3 = P(AXES, None, None)
    return jax.shard_map(
        per_device,
        mesh=mesh,
        in_specs=(split_3,) + (split_2,) * 8 + (split_1, P(), split_1, split_2),
        out_specs=(split_2, split_3),
        check_vma=False,
    )
```

```python
import functools

import jax
import jax.numpy as jnp
from jax import lax
from jax.experimental import pallas as pl
from jax.experimental.pallas import tpu as pltpu
from jax.sharding import PartitionSpec as P

AXES = ("clump", "grp")
LANES = 128
F32, BF16, I32 = jnp.float32, jnp.bfloat16, jnp.int32


def iota(shape, dim):
    return lax.broadcasted_iota(I32, shape, dim)


def split(x):
    high = x.astype(BF16)
    return high, (x - high.astype(F32)).astype(BF16)


def onehot(mask):
    return jnp.where(mask, 1.0, 0.0).astype(BF16)


def dot_nn(a, b):
    return lax.dot_general(a, b, (((1,), (0,)), ((), ())), preferred_element_type=F32)


def dot_nt(a, b):
    return lax.dot_general(a, b, (((1,), (1,)), ((), ())), preferred_element_type=F32)


def lookup(table, index):
    shape = index.shape
    lane, row = index & (LANES - 1), index >> 7
    out = None
    for r in range(table.shape[0]):
        line = jnp.broadcast_to(table[r : r + 1, :], shape)
        got = jnp.take_along_axis(line, lane, axis=1, mode="promise_in_bounds")
        out = got if out is None else jnp.where(row == r, got, out)
    return out


def as_row(x):
    return jnp.concatenate([x[s : s + 1, :] for s in range(x.shape[0])], axis=1)


def order_kernel(before):
    before[...] = onehot(iota(before.shape, 0) < iota(before.shape, 1))


def spread(hots, values):
    high, low = split(values)
    empty = jnp.zeros_like(high)
    count = len(hots)
    rows = [
        jnp.concatenate([empty, empty] * g + [high, low] + [empty, empty] * (count - 1 - g), axis=1)
        for g in range(count)
    ]
    lines = jnp.concatenate([h for hot in hots for h in (hot, hot)], axis=1)
    return dot_nt(lines, jnp.concatenate(rows, axis=0))


def unpack(got, n_dev, lines, stride, nv):
    rows = [got[pl.ds(k, n_dev, stride=stride), :] for k in range(lines)]
    flat = jnp.concatenate(rows, axis=0).T
    groups = [flat[g * nv : (g + 1) * nv] for g in range(LANES // nv)]
    return jnp.concatenate(split(jnp.concatenate(groups, axis=1)), axis=0)


def local_kernel(n_dev, cap, *refs):
    target, pcol, clu, lgrid, pwt, cwt, lwt, pft, scale, flux, frac, count, before, send, kept, slot_out, frac_out = refs
    frac_out[...] = frac[...]
    nv, patches = flux.shape
    cells = target.shape[1]
    groups = LANES // nv
    lines = cap // groups

    goal = target[...]
    owner = goal // cells
    owned = iota((n_dev, cells), 0) == owner
    rank = jnp.sum(jnp.where(owned, dot_nn(onehot(owned), before[...]), 0.0), axis=0, keepdims=True).astype(I32)
    slot = (rank % groups * lines + rank // groups) * n_dev + owner
    local = (goal - owner * cells + 1).astype(F32)
    named = jnp.where(owned, local, 0.0).astype(BF16)
    ids = dot_nt(named, onehot(iota((LANES, cells), 0) == rank)) - 1.0
    send[pl.ds(lines, n_dev, stride=lines + 1), :] = ids

    index = pcol[...]
    land = lookup(clu[...], index)
    home = lookup(lgrid[...], land)
    weight = pwt[...] * lookup(cwt[...], index) * lookup(lwt[...], land)
    position = iota(index.shape, 0) * LANES + iota(index.shape, 1)
    alive = position < count[...]
    slot_out[...] = jnp.where(alive, lookup(slot, home), -1)
    home_row = as_row(jnp.where(alive, home, -1))
    weight_row = as_row(jnp.where(alive, weight, 0.0))
    home_hot = onehot(iota((cells, patches), 0) == home_row)
    w_high, w_low = split(jnp.broadcast_to(weight_row, (16, patches)))
    w_both = jnp.where(iota((16, patches), 0) == 0, w_high, w_low)
    types = scale.shape[0]
    type_hot = onehot(iota((types, patches), 0) == as_row(pft[...]))
    scale_t = jnp.concatenate(split(scale[...]), axis=1).T
    factor = dot_nn(scale_t, type_hot)
    factor = factor[:nv] + factor[nv:]

    scaled = jnp.where(home_row >= 0, flux[...] * factor, 0.0)
    kept[...] = scaled
    high, low = split(scaled * weight_row)
    sums = dot_nt(jnp.concatenate([high, low, w_both], axis=0), home_hot)
    den = sums[2 * nv : 2 * nv + 1] + sums[2 * nv + 1 : 2 * nv + 2]
    mean = (sums[:nv] + sums[nv : 2 * nv]) / jnp.maximum(den, 1.0)
    part = lines * n_dev
    hots = [onehot(iota((part, cells), 0) + g * part == slot) for g in range(groups)]
    out = spread(hots, mean)
    for k in range(lines):
        send[pl.ds(k, n_dev, stride=lines + 1), :] = out[k * n_dev : (k + 1) * n_dev, :]


def owner_kernel(n_dev, cap, got, frac, field, send, merged_out):
    nv, cells = field.shape
    groups = LANES // nv
    lines = cap // groups
    ids = got[pl.ds(lines, n_dev, stride=lines + 1), :]
    lane = iota((n_dev, cells), 1).astype(F32)
    hots = []
    for g in range(groups):
        named = [ids[:, k * groups + g : k * groups + g + 1] for k in range(lines)]
        hots.append(jnp.concatenate([onehot(lane == column) for column in named], axis=0))
    means = unpack(got, n_dev, lines, lines + 1, nv)
    placed = dot_nn(means, jnp.concatenate(hots, axis=0))
    part = frac[...]
    merged = part * (placed[:nv] + placed[nv:]) + (1.0 - part) * field[...]
    merged_out[...] = merged
    out = spread(hots, merged)
    for k in range(lines):
        send[pl.ds(k, n_dev, stride=lines), :] = out[k * n_dev : (k + 1) * n_dev, :]


def finish_kernel(n_dev, cap, got, slot, kept, merged, merged_out, anomaly_out):
    merged_out[...] = merged[...]
    nv, patches = kept.shape
    lines = cap * nv // LANES
    replies = unpack(got, n_dev, lines, lines, nv)
    hot = onehot(iota((n_dev * cap, patches), 0) == as_row(slot[...]))
    picked = dot_nn(replies, hot)
    anomaly_out[...] = kept[...] - (picked[:nv] + picked[nv:])


def shape(dims, dtype=F32):
    return jax.ShapeDtypeStruct(dims, dtype)


VMEM = pl.BlockSpec(memory_space=pltpu.VMEM)


def call(body, outs, in_specs, flops, scratch=()):
    return pl.pallas_call(
        body,
        out_shape=outs,
        in_specs=in_specs,
        out_specs=[VMEM] * len(outs),
        scratch_shapes=list(scratch),
        compiler_params=pltpu.CompilerParams(vmem_limit_bytes=16 << 20),
        cost_estimate=pl.CostEstimate(flops=flops, bytes_accessed=1 << 20, transcendentals=0),
    )


def per_device(
    flux,
    patch_pft,
    patch_wt,
    patch_col,
    col_wt,
    col_lu,
    lu_wt,
    lu_grid,
    cell_target,
    patch_count,
    pft_scale,
    cpl_frac,
    cpl_field,
):
    n_dev = lax.axis_size("clump") * lax.axis_size("grp")
    patches, nv = flux.shape[1:]
    cells = cell_target.shape[1]
    cap = max(2, 2 * cells // n_dev)
    lines = cap * nv // LANES
    lanes = lambda x: x.reshape(-1, LANES)

    def exchange(x):
        rows = x.shape[0] // n_dev
        x = x.reshape(n_dev, 1, rows * LANES)
        return lax.all_to_all(x, AXES, split_axis=0, concat_axis=0, tiled=True).reshape(-1, LANES)

    inputs = [
        cell_target,
        lanes(patch_col),
        lanes(col_lu),
        lanes(lu_grid),
        lanes(patch_wt),
        lanes(col_wt),
        lanes(lu_wt),
        lanes(patch_pft),
        pft_scale,
        flux[0].T,
        cpl_frac.reshape(1, cells),
        patch_count.reshape(1, 1),
    ]
    (before,) = call(order_kernel, [shape((cells, cells), BF16)], [], 1 << 33)()
    inputs.append(before)
    send, kept, slot, frac = call(
        functools.partial(local_kernel, n_dev, cap),
        [
            shape((n_dev * (lines + 1), LANES)),
            shape((nv, patches)),
            shape((patches // LANES, LANES), I32),
            shape((1, cells)),
        ],
        [VMEM] * len(inputs),
        1 << 26,
    )(*inputs)
    reply, merged = call(
        functools.partial(owner_kernel, n_dev, cap),
        [shape((n_dev * lines, LANES)), shape((nv, cells))],
        [VMEM] * 3,
        1 << 26,
    )(exchange(send), frac, cpl_field.T)
    merged, anomaly = call(
        functools.partial(finish_kernel, n_dev, cap),
        [shape((nv, cells)), shape((nv, patches))],
        [VMEM] * 4,
        1 << 26,
    )(exchange(reply), slot, kept, merged)
    return merged.T, anomaly.T[None]


def solution(mesh):
    split_1 = P(AXES)
    split_2 = P(AXES, None)
    split_3 = P(AXES, None, None)
    return jax.shard_map(
        per_device,
        mesh=mesh,
        in_specs=(split_3,) + (split_2,) * 8 + (split_1, P(), split_1, split_2),
        out_specs=(split_2, split_3),
        check_vma=False,
    )
```

```python
import functools

import jax
import jax.numpy as jnp
from jax import lax
from jax.experimental import pallas as pl
from jax.experimental.pallas import tpu as pltpu
from jax.sharding import PartitionSpec as P

AXES = ("clump", "grp")
LANES = 128
PIECE = 256
F32, BF16, I32 = jnp.float32, jnp.bfloat16, jnp.int32


def iota(shape, dim):
    return lax.broadcasted_iota(I32, shape, dim)


def split(x):
    high = x.astype(BF16)
    return high, (x - high.astype(F32)).astype(BF16)


def onehot(mask):
    return jnp.where(mask, 1.0, 0.0).astype(BF16)


def dot_nn(a, b):
    return lax.dot_general(a, b, (((1,), (0,)), ((), ())), preferred_element_type=F32)


def dot_nt(a, b):
    return lax.dot_general(a, b, (((1,), (1,)), ((), ())), preferred_element_type=F32)


def lookup(table, index):
    shape = index.shape
    lane, row = index & (LANES - 1), index >> 7
    out = None
    for r in range(table.shape[0]):
        line = jnp.broadcast_to(table[r : r + 1, :], shape)
        got = jnp.take_along_axis(line, lane, axis=1, mode="promise_in_bounds")
        out = got if out is None else jnp.where(row == r, got, out)
    return out


def as_row(x):
    return jnp.concatenate([x[s : s + 1, :] for s in range(x.shape[0])], axis=1)


def order_kernel(before):
    before[...] = onehot(iota(before.shape, 0) < iota(before.shape, 1))


def spread(hots, values):
    high, low = split(values)
    empty = jnp.zeros_like(high)
    count = len(hots)
    rows = [
        jnp.concatenate([empty, empty] * g + [high, low] + [empty, empty] * (count - 1 - g), axis=1)
        for g in range(count)
    ]
    lines = jnp.concatenate([h for hot in hots for h in (hot, hot)], axis=1)
    return dot_nt(lines, jnp.concatenate(rows, axis=0))


def unpack(got, n_dev, lines, stride, nv):
    rows = [got[pl.ds(k, n_dev, stride=stride), :] for k in range(lines)]
    flat = jnp.concatenate(rows, axis=0).T
    groups = [flat[g * nv : (g + 1) * nv] for g in range(LANES // nv)]
    return jnp.concatenate(split(jnp.concatenate(groups, axis=1)), axis=0)


def prepare_kernel(
    n_dev,
    cap,
    pcol,
    clu,
    lgrid,
    pwt,
    cwt,
    lwt,
    count,
    target,
    pft,
    scale,
    frac,
    before,
    live_scale,
    sum_scale,
    home_hot,
    weights,
    slot_hot,
    ids,
    slot_out,
    frac_out,
):
    frac_out[...] = frac[...]
    cells, patches = home_hot.shape
    nv = live_scale.shape[0]
    groups = LANES // nv
    lines = cap // groups

    index = pcol[...]
    land = lookup(clu[...], index)
    home = lookup(lgrid[...], land)
    weight = pwt[...] * lookup(cwt[...], index) * lookup(lwt[...], land)
    position = iota(index.shape, 0) * LANES + iota(index.shape, 1)
    alive = position < count[...]

    goal = target[...]
    owner = goal // cells
    owned = iota((n_dev, cells), 0) == owner
    rank = jnp.sum(jnp.where(owned, dot_nn(onehot(owned), before[...]), 0.0), axis=0, keepdims=True)
    rank = rank.astype(I32)
    slot = (rank % groups * lines + rank // groups) * n_dev + owner
    local = (goal - owner * cells + 1).astype(F32)
    named = jnp.where(owned, local, 0.0).astype(BF16)
    ids[...] = dot_nt(named, onehot(iota((LANES, cells), 0) == rank)) - 1.0
    slot_hot[...] = onehot(iota(slot_hot.shape, 0) == slot)
    slot_out[...] = jnp.where(alive, lookup(slot, home), -1)

    types = scale.shape[0]
    type_hot = onehot(iota((types, patches), 0) == as_row(pft[...]))
    scale_t = jnp.concatenate(split(scale[...]), axis=1).T
    factor = dot_nn(scale_t, type_hot)
    factor = factor[:nv] + factor[nv:]
    home_row = as_row(jnp.where(alive, home, -1))
    weight_row = as_row(jnp.where(alive, weight, 0.0))
    live_scale[...] = jnp.where(home_row >= 0, factor, 0.0)
    sum_scale[...] = factor * weight_row
    home_hot[...] = onehot(iota((cells, patches), 0) == home_row)
    w_high, w_low = split(jnp.broadcast_to(weight_row, weights.shape))
    weights[...] = jnp.where(iota(weights.shape, 0) == 0, w_high, w_low)


def local_kernel(
    n_dev, flux, live_scale, sum_scale, home_hot, weights, slot_hot, ids, send, kept
):
    nv = flux.shape[0]
    groups = LANES // nv
    part = slot_hot.shape[0] // groups
    lines = part // n_dev
    values = flux[...]
    high, low = split(values * sum_scale[...])
    sums = dot_nt(jnp.concatenate([high, low, weights[...]], axis=0), home_hot[...])
    kept[...] = values * live_scale[...]
    send[pl.ds(lines, n_dev, stride=lines + 1), :] = ids[...]
    den = sums[2 * nv : 2 * nv + 1] + sums[2 * nv + 1 : 2 * nv + 2]
    mean = (sums[:nv] + sums[nv : 2 * nv]) / jnp.maximum(den, 1.0)
    out = spread([slot_hot[g * part : (g + 1) * part, :] for g in range(groups)], mean)
    for k in range(lines):
        send[pl.ds(k, n_dev, stride=lines + 1), :] = out[k * n_dev : (k + 1) * n_dev, :]


def owner_kernel(n_dev, cap, got, frac, field, send, merged_out):
    nv, cells = field.shape
    groups = LANES // nv
    lines = cap // groups
    ids = got[pl.ds(lines, n_dev, stride=lines + 1), :]
    lane = iota((n_dev, cells), 1).astype(F32)
    hots = []
    for g in range(groups):
        named = [ids[:, k * groups + g : k * groups + g + 1] for k in range(lines)]
        hots.append(jnp.concatenate([onehot(lane == column) for column in named], axis=0))
    part = frac[...]
    rest = (1.0 - part) * field[...]
    own = spread(hots, jnp.broadcast_to(part, (nv, cells)))
    other = spread(hots, rest)
    for k in range(lines):
        at = slice(k * n_dev, (k + 1) * n_dev)
        row = got[pl.ds(k, n_dev, stride=lines + 1), :]
        send[pl.ds(k, n_dev, stride=lines), :] = own[at, :] * row + other[at, :]
    means = unpack(got, n_dev, lines, lines + 1, nv)
    placed = dot_nn(means, jnp.concatenate(hots, axis=0))
    merged_out[...] = part * (placed[:nv] + placed[nv:]) + rest


def finish_kernel(n_dev, cap, got, slot, kept, merged, merged_out, anomaly_out, buffer, sem):
    nv, patches = kept.shape
    pieces = buffer.shape[1] // PIECE
    copies = [pltpu.make_async_copy(merged, merged_out, sem.at[pieces])]
    copies[0].start()
    lines = cap * nv // LANES
    replies = unpack(got, n_dev, lines, lines, nv)
    row = as_row(slot[...])
    for c in range(pieces):
        at = slice(c * PIECE, (c + 1) * PIECE)
        hot = onehot(iota((n_dev * cap, PIECE), 0) == row[:, at])
        picked = dot_nn(replies, hot)
        buffer[:, at] = kept[:, at] - (picked[:nv] + picked[nv:])
        copies.append(pltpu.make_async_copy(buffer.at[:, at], anomaly_out.at[:, at], sem.at[c]))
        copies[-1].start()
    for copy in copies:
        copy.wait()


def shape(dims, dtype=F32):
    return jax.ShapeDtypeStruct(dims, dtype)


VMEM = pl.BlockSpec(memory_space=pltpu.VMEM)
HBM = pl.BlockSpec(memory_space=pltpu.HBM)


def call(body, outs, in_specs, flops, scratch=(), space=None):
    return pl.pallas_call(
        body,
        out_shape=outs,
        in_specs=in_specs,
        out_specs=[space or VMEM] * len(outs),
        scratch_shapes=list(scratch),
        compiler_params=pltpu.CompilerParams(vmem_limit_bytes=16 << 20),
        cost_estimate=pl.CostEstimate(flops=flops, bytes_accessed=1 << 20, transcendentals=0),
    )


def per_device(
    flux,
    patch_pft,
    patch_wt,
    patch_col,
    col_wt,
    col_lu,
    lu_wt,
    lu_grid,
    cell_target,
    patch_count,
    pft_scale,
    cpl_frac,
    cpl_field,
):
    n_dev = lax.axis_size("clump") * lax.axis_size("grp")
    patches, nv = flux.shape[1:]
    cells = cell_target.shape[1]
    cap = max(2, 2 * cells // n_dev)
    lines = cap * nv // LANES
    lanes = lambda x: x.reshape(-1, LANES)

    def exchange(x):
        rows = x.shape[0] // n_dev
        x = x.reshape(n_dev, 1, rows * LANES)
        return lax.all_to_all(x, AXES, split_axis=0, concat_axis=0, tiled=True).reshape(-1, LANES)

    (before,) = call(order_kernel, [shape((cells, cells), BF16)], [], 1 << 29)()
    *plan, slot, frac = call(
        functools.partial(prepare_kernel, n_dev, cap),
        [
            shape((nv, patches)),
            shape((nv, patches)),
            shape((cells, patches), BF16),
            shape((16, patches), BF16),
            shape((n_dev * cap, cells), BF16),
            shape((n_dev, LANES)),
            shape((patches // LANES, LANES), I32),
            shape((1, cells)),
        ],
        [VMEM] * 12,
        1 << 26,
    )(
        lanes(patch_col),
        lanes(col_lu),
        lanes(lu_grid),
        lanes(patch_wt),
        lanes(col_wt),
        lanes(lu_wt),
        patch_count.reshape(1, 1),
        cell_target,
        lanes(patch_pft),
        pft_scale,
        cpl_frac.reshape(1, cells),
        before,
    )
    send, kept = call(
        functools.partial(local_kernel, n_dev),
        [shape((n_dev * (lines + 1), LANES)), shape((nv, patches))],
        [VMEM] * 7,
        1 << 26,
    )(flux[0].T, *plan)
    reply, merged = call(
        functools.partial(owner_kernel, n_dev, cap),
        [shape((n_dev * lines, LANES)), shape((nv, cells))],
        [VMEM] * 3,
        1 << 26,
    )(exchange(send), frac, cpl_field.T)
    merged, anomaly = call(
        functools.partial(finish_kernel, n_dev, cap),
        [shape((nv, cells)), shape((nv, patches))],
        [VMEM] * 4,
        1 << 26,
        [pltpu.VMEM((nv, patches), F32), pltpu.SemaphoreType.DMA((patches // PIECE + 1,))],
        HBM,
    )(exchange(reply), slot, kept, merged)
    return merged.T, anomaly.T[None]


def solution(mesh):
    split_1 = P(AXES)
    split_2 = P(AXES, None)
    split_3 = P(AXES, None, None)
    return jax.shard_map(
        per_device,
        mesh=mesh,
        in_specs=(split_3,) + (split_2,) * 8 + (split_1, P(), split_1, split_2),
        out_specs=(split_2, split_3),
        check_vma=False,
    )
```

```python
import functools

import jax
import jax.numpy as jnp
from jax import lax
from jax.experimental import pallas as pl
from jax.experimental.pallas import tpu as pltpu
from jax.sharding import PartitionSpec as P

AXES = ("clump", "grp")
ORDER = ("grp", "clump")
LANES = 128
PIECE = 256
F32, BF16, I32 = jnp.float32, jnp.bfloat16, jnp.int32


def iota(shape, dim):
    return lax.broadcasted_iota(I32, shape, dim)


def split(x):
    high = x.astype(BF16)
    return high, (x - high.astype(F32)).astype(BF16)


def onehot(mask):
    return jnp.where(mask, 1.0, 0.0).astype(BF16)


def dot_nn(a, b):
    return lax.dot_general(a, b, (((1,), (0,)), ((), ())), preferred_element_type=F32)


def dot_nt(a, b):
    return lax.dot_general(a, b, (((1,), (1,)), ((), ())), preferred_element_type=F32)


def lookup(table, index):
    shape = index.shape
    lane, row = index & (LANES - 1), index >> 7
    out = None
    for r in range(table.shape[0]):
        line = jnp.broadcast_to(table[r : r + 1, :], shape)
        got = jnp.take_along_axis(line, lane, axis=1, mode="promise_in_bounds")
        out = got if out is None else jnp.where(row == r, got, out)
    return out


def as_row(x):
    return jnp.concatenate([x[s : s + 1, :] for s in range(x.shape[0])], axis=1)


def order_kernel(before):
    before[...] = onehot(iota(before.shape, 0) < iota(before.shape, 1))


def spread(hots, values):
    high, low = split(values)
    empty = jnp.zeros_like(high)
    count = len(hots)
    rows = [
        jnp.concatenate([empty, empty] * g + [high, low] + [empty, empty] * (count - 1 - g), axis=1)
        for g in range(count)
    ]
    lines = jnp.concatenate([h for hot in hots for h in (hot, hot)], axis=1)
    return dot_nt(lines, jnp.concatenate(rows, axis=0))


def unpack(got, n_dev, lines, stride, nv):
    rows = [got[pl.ds(k, n_dev, stride=stride), :] for k in range(lines)]
    flat = jnp.concatenate(rows, axis=0).T
    groups = [flat[g * nv : (g + 1) * nv] for g in range(LANES // nv)]
    return jnp.concatenate(split(jnp.concatenate(groups, axis=1)), axis=0)


def prepare_kernel(
    n_clump,
    n_group,
    cap,
    pcol,
    clu,
    lgrid,
    pwt,
    cwt,
    lwt,
    count,
    target,
    pft,
    scale,
    frac,
    before,
    live_scale,
    sum_scale,
    home_hot,
    weights,
    slot_hot,
    ids,
    slot_out,
    frac_out,
):
    frac_out[...] = frac[...]
    n_dev = n_clump * n_group
    cells, patches = home_hot.shape
    nv = live_scale.shape[0]
    groups = LANES // nv
    lines = cap // groups

    index = pcol[...]
    land = lookup(clu[...], index)
    home = lookup(lgrid[...], land)
    weight = pwt[...] * lookup(cwt[...], index) * lookup(lwt[...], land)
    position = iota(index.shape, 0) * LANES + iota(index.shape, 1)
    alive = position < count[...]

    goal = target[...]
    owner = goal // cells
    seat = owner % n_group * n_clump + owner // n_group
    owned = iota((n_dev, cells), 0) == seat
    rank = jnp.sum(jnp.where(owned, dot_nn(onehot(owned), before[...]), 0.0), axis=0, keepdims=True)
    rank = rank.astype(I32)
    slot = (rank % groups * lines + rank // groups) * n_dev + seat
    local = (goal - owner * cells + 1).astype(F32)
    named = jnp.where(owned, local, 0.0).astype(BF16)
    ids[...] = dot_nt(named, onehot(iota((LANES, cells), 0) == rank)) - 1.0
    slot_hot[...] = onehot(iota(slot_hot.shape, 0) == slot)
    slot_out[...] = jnp.where(alive, lookup(slot, home), -1)

    types = scale.shape[0]
    type_hot = onehot(iota((types, patches), 0) == as_row(pft[...]))
    scale_t = jnp.concatenate(split(scale[...]), axis=1).T
    factor = dot_nn(scale_t, type_hot)
    factor = factor[:nv] + factor[nv:]
    home_row = as_row(jnp.where(alive, home, -1))
    weight_row = as_row(jnp.where(alive, weight, 0.0))
    live_scale[...] = jnp.where(home_row >= 0, factor, 0.0)
    sum_scale[...] = factor * weight_row
    home_hot[...] = onehot(iota((cells, patches), 0) == home_row)
    w_high, w_low = split(jnp.broadcast_to(weight_row, weights.shape))
    weights[...] = jnp.where(iota(weights.shape, 0) == 0, w_high, w_low)


def local_kernel(
    n_dev, flux, live_scale, sum_scale, home_hot, weights, slot_hot, ids, send, kept
):
    nv = flux.shape[0]
    groups = LANES // nv
    part = slot_hot.shape[0] // groups
    lines = part // n_dev
    values = flux[...]
    high, low = split(values * sum_scale[...])
    sums = dot_nt(jnp.concatenate([high, low, weights[...]], axis=0), home_hot[...])
    kept[...] = values * live_scale[...]
    send[pl.ds(lines, n_dev, stride=lines + 1), :] = ids[...]
    den = sums[2 * nv : 2 * nv + 1] + sums[2 * nv + 1 : 2 * nv + 2]
    mean = (sums[:nv] + sums[nv : 2 * nv]) / jnp.maximum(den, 1.0)
    out = spread([slot_hot[g * part : (g + 1) * part, :] for g in range(groups)], mean)
    for k in range(lines):
        send[pl.ds(k, n_dev, stride=lines + 1), :] = out[k * n_dev : (k + 1) * n_dev, :]


def owner_kernel(n_dev, cap, got, frac, field, send, merged_out):
    nv, cells = field.shape
    groups = LANES // nv
    lines = cap // groups
    ids = got[pl.ds(lines, n_dev, stride=lines + 1), :]
    lane = iota((n_dev, cells), 1).astype(F32)
    hots = []
    for g in range(groups):
        named = [ids[:, k * groups + g : k * groups + g + 1] for k in range(lines)]
        hots.append(jnp.concatenate([onehot(lane == column) for column in named], axis=0))
    part = frac[...]
    rest = (1.0 - part) * field[...]
    own = spread(hots, jnp.broadcast_to(part, (nv, cells)))
    other = spread(hots, rest)
    for k in range(lines):
        at = slice(k * n_dev, (k + 1) * n_dev)
        row = got[pl.ds(k, n_dev, stride=lines + 1), :]
        send[pl.ds(k, n_dev, stride=lines), :] = own[at, :] * row + other[at, :]
    means = unpack(got, n_dev, lines, lines + 1, nv)
    placed = dot_nn(means, jnp.concatenate(hots, axis=0))
    merged_out[...] = part * (placed[:nv] + placed[nv:]) + rest


def finish_kernel(n_dev, cap, got, slot, kept, merged, merged_out, anomaly_out, buffer, sem):
    nv, patches = kept.shape
    pieces = buffer.shape[1] // PIECE
    copies = [pltpu.make_async_copy(merged, merged_out, sem.at[pieces])]
    copies[0].start()
    lines = cap * nv // LANES
    replies = unpack(got, n_dev, lines, lines, nv)
    row = as_row(slot[...])
    for c in range(pieces):
        at = slice(c * PIECE, (c + 1) * PIECE)
        hot = onehot(iota((n_dev * cap, PIECE), 0) == row[:, at])
        picked = dot_nn(replies, hot)
        buffer[:, at] = kept[:, at] - (picked[:nv] + picked[nv:])
        copies.append(pltpu.make_async_copy(buffer.at[:, at], anomaly_out.at[:, at], sem.at[c]))
        copies[-1].start()
    for copy in copies:
        copy.wait()


def shape(dims, dtype=F32):
    return jax.ShapeDtypeStruct(dims, dtype)


VMEM = pl.BlockSpec(memory_space=pltpu.VMEM)
HBM = pl.BlockSpec(memory_space=pltpu.HBM)


def call(body, outs, in_specs, flops, scratch=(), space=None):
    return pl.pallas_call(
        body,
        out_shape=outs,
        in_specs=in_specs,
        out_specs=[space or VMEM] * len(outs),
        scratch_shapes=list(scratch),
        compiler_params=pltpu.CompilerParams(vmem_limit_bytes=16 << 20),
        cost_estimate=pl.CostEstimate(flops=flops, bytes_accessed=1 << 20, transcendentals=0),
    )


def per_device(
    flux,
    patch_pft,
    patch_wt,
    patch_col,
    col_wt,
    col_lu,
    lu_wt,
    lu_grid,
    cell_target,
    patch_count,
    pft_scale,
    cpl_frac,
    cpl_field,
):
    n_clump, n_group = lax.axis_size("clump"), lax.axis_size("grp")
    n_dev = n_clump * n_group
    patches, nv = flux.shape[1:]
    cells = cell_target.shape[1]
    cap = max(2, 2 * cells // n_dev)
    lines = cap * nv // LANES
    lanes = lambda x: x.reshape(-1, LANES)

    def exchange(x):
        rows = x.shape[0] // n_dev
        whole = rows & (rows - 1) == 0
        x = x.reshape(n_dev, rows, LANES) if whole else x.reshape(n_dev, 1, rows * LANES)
        return lax.all_to_all(x, ORDER, split_axis=0, concat_axis=0, tiled=True).reshape(-1, LANES)

    (before,) = call(order_kernel, [shape((cells, cells), BF16)], [], 1 << 29)()
    *plan, slot, frac = call(
        functools.partial(prepare_kernel, n_clump, n_group, cap),
        [
            shape((nv, patches)),
            shape((nv, patches)),
            shape((cells, patches), BF16),
            shape((16, patches), BF16),
            shape((n_dev * cap, cells), BF16),
            shape((n_dev, LANES)),
            shape((patches // LANES, LANES), I32),
            shape((1, cells)),
        ],
        [VMEM] * 12,
        1 << 26,
    )(
        lanes(patch_col),
        lanes(col_lu),
        lanes(lu_grid),
        lanes(patch_wt),
        lanes(col_wt),
        lanes(lu_wt),
        patch_count.reshape(1, 1),
        cell_target,
        lanes(patch_pft),
        pft_scale,
        cpl_frac.reshape(1, cells),
        before,
    )
    send, kept = call(
        functools.partial(local_kernel, n_dev),
        [shape((n_dev * (lines + 1), LANES)), shape((nv, patches))],
        [VMEM] * 7,
        1 << 26,
    )(flux[0].T, *plan)
    reply, merged = call(
        functools.partial(owner_kernel, n_dev, cap),
        [shape((n_dev * lines, LANES)), shape((nv, cells))],
        [VMEM] * 3,
        1 << 26,
    )(exchange(send), frac, cpl_field.T)
    merged, anomaly = call(
        functools.partial(finish_kernel, n_dev, cap),
        [shape((nv, cells)), shape((nv, patches))],
        [VMEM] * 4,
        1 << 26,
        [pltpu.VMEM((nv, patches), F32), pltpu.SemaphoreType.DMA((patches // PIECE + 1,))],
        HBM,
    )(exchange(reply), slot, kept, merged)
    return merged.T, anomaly.T[None]


def solution(mesh):
    split_1 = P(AXES)
    split_2 = P(AXES, None)
    split_3 = P(AXES, None, None)
    return jax.shard_map(
        per_device,
        mesh=mesh,
        in_specs=(split_3,) + (split_2,) * 8 + (split_1, P(), split_1, split_2),
        out_specs=(split_2, split_3),
        check_vma=False,
    )
```

```python
import functools

import jax
import jax.numpy as jnp
from jax import lax
from jax.experimental import pallas as pl
from jax.experimental.pallas import tpu as pltpu
from jax.sharding import PartitionSpec as P

AXES = ("clump", "grp")
ORDER = ("grp", "clump")
LANES = 128
PIECE = 256
F32, BF16, I32 = jnp.float32, jnp.bfloat16, jnp.int32


def iota(shape, dim):
    return lax.broadcasted_iota(I32, shape, dim)


def split(x):
    high = x.astype(BF16)
    return high, (x - high.astype(F32)).astype(BF16)


def onehot(mask):
    return jnp.where(mask, 1.0, 0.0).astype(BF16)


def dot_nn(a, b):
    return lax.dot_general(a, b, (((1,), (0,)), ((), ())), preferred_element_type=F32)


def dot_nt(a, b):
    return lax.dot_general(a, b, (((1,), (1,)), ((), ())), preferred_element_type=F32)


def lookup(table, index):
    shape = index.shape
    lane, row = index & (LANES - 1), index >> 7
    out = None
    for r in range(table.shape[0]):
        line = jnp.broadcast_to(table[r : r + 1, :], shape)
        got = jnp.take_along_axis(line, lane, axis=1, mode="promise_in_bounds")
        out = got if out is None else jnp.where(row == r, got, out)
    return out


def as_row(x):
    return jnp.concatenate([x[s : s + 1, :] for s in range(x.shape[0])], axis=1)


def order_kernel(before):
    before[...] = onehot(iota(before.shape, 0) < iota(before.shape, 1))


def spread(hots, values):
    high, low = split(values)
    empty = jnp.zeros_like(high)
    count = len(hots)
    rows = [
        jnp.concatenate([empty, empty] * g + [high, low] + [empty, empty] * (count - 1 - g), axis=1)
        for g in range(count)
    ]
    lines = jnp.concatenate([h for hot in hots for h in (hot, hot)], axis=1)
    return dot_nt(lines, jnp.concatenate(rows, axis=0))


def unpack(got, n_dev, lines, stride, nv):
    rows = [got[pl.ds(k, n_dev, stride=stride), :] for k in range(lines)]
    flat = jnp.concatenate(rows, axis=0).T
    groups = [flat[g * nv : (g + 1) * nv] for g in range(LANES // nv)]
    return jnp.concatenate(split(jnp.concatenate(groups, axis=1)), axis=0)


def prepare_kernel(
    n_clump,
    n_group,
    cap,
    pcol,
    clu,
    lgrid,
    pwt,
    cwt,
    lwt,
    count,
    target,
    pft,
    scale,
    frac,
    before,
    factor_out,
    weight_out,
    home_hot,
    weights,
    slot_hot,
    ids,
    slot_out,
    frac_out,
):
    frac_out[...] = frac[...]
    n_dev = n_clump * n_group
    cells, patches = home_hot.shape
    nv = factor_out.shape[0]
    groups = LANES // nv
    lines = cap // groups

    index = pcol[...]
    land = lookup(clu[...], index)
    home = lookup(lgrid[...], land)
    weight = pwt[...] * lookup(cwt[...], index) * lookup(lwt[...], land)
    position = iota(index.shape, 0) * LANES + iota(index.shape, 1)
    alive = position < count[...]

    goal = target[...]
    owner = goal // cells
    seat = owner % n_group * n_clump + owner // n_group
    owned = iota((n_dev, cells), 0) == seat
    rank = jnp.sum(jnp.where(owned, dot_nn(onehot(owned), before[...]), 0.0), axis=0, keepdims=True)
    rank = rank.astype(I32)
    slot = (rank % groups * lines + rank // groups) * n_dev + seat
    local = (goal - owner * cells + 1).astype(F32)
    named = jnp.where(owned, local, 0.0).astype(BF16)
    ids[...] = dot_nt(named, onehot(iota((LANES, cells), 0) == rank)) - 1.0
    slot_hot[...] = onehot(iota(slot_hot.shape, 0) == slot)
    slot_out[...] = jnp.where(alive, lookup(slot, home), -1)

    types = scale.shape[0]
    type_hot = onehot(iota((types, patches), 0) == as_row(pft[...]))
    scale_t = jnp.concatenate(split(scale[...]), axis=1).T
    factor = dot_nn(scale_t, type_hot)
    home_row = as_row(jnp.where(alive, home, -1))
    weight_row = as_row(jnp.where(alive, weight, 0.0))
    weight_out[...] = weight_row
    factor_out[...] = jnp.where(home_row >= 0, factor[:nv] + factor[nv:], 0.0)
    home_hot[...] = onehot(iota((cells, patches), 0) == home_row)
    w_high, w_low = split(jnp.broadcast_to(weight_row, weights.shape))
    weights[...] = jnp.where(iota(weights.shape, 0) == 0, w_high, w_low)


def local_kernel(
    n_dev, flux, factor, weight, home_hot, weights, slot_hot, ids, send, kept
):
    nv = flux.shape[0]
    groups = LANES // nv
    part = slot_hot.shape[0] // groups
    lines = part // n_dev
    scaled = flux[...] * factor[...]
    high, low = split(scaled * weight[...])
    sums = dot_nt(jnp.concatenate([high, low, weights[...]], axis=0), home_hot[...])
    kept[...] = scaled
    send[pl.ds(lines, n_dev, stride=lines + 1), :] = ids[...]
    den = sums[2 * nv : 2 * nv + 1] + sums[2 * nv + 1 : 2 * nv + 2]
    mean = (sums[:nv] + sums[nv : 2 * nv]) / jnp.maximum(den, 1.0)
    out = spread([slot_hot[g * part : (g + 1) * part, :] for g in range(groups)], mean)
    for k in range(lines):
        send[pl.ds(k, n_dev, stride=lines + 1), :] = out[k * n_dev : (k + 1) * n_dev, :]


def owner_kernel(n_dev, cap, got, frac, field, send, merged_out):
    nv, cells = field.shape
    groups = LANES // nv
    lines = cap // groups
    ids = got[pl.ds(lines, n_dev, stride=lines + 1), :]
    lane = iota((n_dev, cells), 1).astype(F32)
    hots = []
    for g in range(groups):
        named = [ids[:, k * groups + g : k * groups + g + 1] for k in range(lines)]
        hots.append(jnp.concatenate([onehot(lane == column) for column in named], axis=0))
    part = frac[...]
    rest = (1.0 - part) * field[...]
    own = spread(hots, jnp.broadcast_to(part, (nv, cells)))
    other = spread(hots, rest)
    for k in range(lines):
        at = slice(k * n_dev, (k + 1) * n_dev)
        row = got[pl.ds(k, n_dev, stride=lines + 1), :]
        send[pl.ds(k, n_dev, stride=lines), :] = own[at, :] * row + other[at, :]
    means = unpack(got, n_dev, lines, lines + 1, nv)
    placed = dot_nn(means, jnp.concatenate(hots, axis=0))
    merged_out[...] = part * (placed[:nv] + placed[nv:]) + rest


def finish_kernel(n_dev, cap, got, slot, kept, merged, merged_out, anomaly_out, buffer, sem):
    nv, patches = kept.shape
    pieces = buffer.shape[1] // PIECE
    copies = [pltpu.make_async_copy(merged, merged_out, sem.at[pieces])]
    copies[0].start()
    lines = cap * nv // LANES
    replies = unpack(got, n_dev, lines, lines, nv)
    row = as_row(slot[...])
    for c in range(pieces):
        at = slice(c * PIECE, (c + 1) * PIECE)
        hot = onehot(iota((n_dev * cap, PIECE), 0) == row[:, at])
        picked = dot_nn(replies, hot)
        buffer[:, at] = kept[:, at] - (picked[:nv] + picked[nv:])
        copies.append(pltpu.make_async_copy(buffer.at[:, at], anomaly_out.at[:, at], sem.at[c]))
        copies[-1].start()
    for copy in copies:
        copy.wait()


def shape(dims, dtype=F32):
    return jax.ShapeDtypeStruct(dims, dtype)


VMEM = pl.BlockSpec(memory_space=pltpu.VMEM)
HBM = pl.BlockSpec(memory_space=pltpu.HBM)


def call(body, outs, in_specs, flops, scratch=(), space=None):
    return pl.pallas_call(
        body,
        out_shape=outs,
        in_specs=in_specs,
        out_specs=[space or VMEM] * len(outs),
        scratch_shapes=list(scratch),
        compiler_params=pltpu.CompilerParams(vmem_limit_bytes=16 << 20),
        cost_estimate=pl.CostEstimate(flops=flops, bytes_accessed=1 << 20, transcendentals=0),
    )


def per_device(
    flux,
    patch_pft,
    patch_wt,
    patch_col,
    col_wt,
    col_lu,
    lu_wt,
    lu_grid,
    cell_target,
    patch_count,
    pft_scale,
    cpl_frac,
    cpl_field,
):
    n_clump, n_group = lax.axis_size("clump"), lax.axis_size("grp")
    n_dev = n_clump * n_group
    patches, nv = flux.shape[1:]
    cells = cell_target.shape[1]
    cap = max(2, 2 * cells // n_dev)
    lines = cap * nv // LANES
    lanes = lambda x: x.reshape(-1, LANES)

    def exchange(x):
        rows = x.shape[0] // n_dev
        whole = rows & (rows - 1) == 0
        x = x.reshape(n_dev, rows, LANES) if whole else x.reshape(n_dev, 1, rows * LANES)
        return lax.all_to_all(x, ORDER, split_axis=0, concat_axis=0, tiled=True).reshape(-1, LANES)

    (before,) = call(order_kernel, [shape((cells, cells), BF16)], [], 1 << 29)()
    *plan, slot, frac = call(
        functools.partial(prepare_kernel, n_clump, n_group, cap),
        [
            shape((nv, patches)),
            shape((1, patches)),
            shape((cells, patches), BF16),
            shape((16, patches), BF16),
            shape((n_dev * cap, cells), BF16),
            shape((n_dev, LANES)),
            shape((patches // LANES, LANES), I32),
            shape((1, cells)),
        ],
        [VMEM] * 12,
        1 << 26,
    )(
        lanes(patch_col),
        lanes(col_lu),
        lanes(lu_grid),
        lanes(patch_wt),
        lanes(col_wt),
        lanes(lu_wt),
        patch_count.reshape(1, 1),
        cell_target,
        lanes(patch_pft),
        pft_scale,
        cpl_frac.reshape(1, cells),
        before,
    )
    send, kept = call(
        functools.partial(local_kernel, n_dev),
        [shape((n_dev * (lines + 1), LANES)), shape((nv, patches))],
        [VMEM] * 7,
        1 << 26,
    )(flux[0].T, *plan)
    reply, merged = call(
        functools.partial(owner_kernel, n_dev, cap),
        [shape((n_dev * lines, LANES)), shape((nv, cells))],
        [VMEM] * 3,
        1 << 26,
    )(exchange(send), frac, cpl_field.T)
    merged, anomaly = call(
        functools.partial(finish_kernel, n_dev, cap),
        [shape((nv, cells)), shape((nv, patches))],
        [VMEM] * 4,
        1 << 26,
        [pltpu.VMEM((nv, patches), F32), pltpu.SemaphoreType.DMA((patches // PIECE + 1,))],
        HBM,
    )(exchange(reply), slot, kept, merged)
    return merged.T, anomaly.T[None]


def solution(mesh):
    split_1 = P(AXES)
    split_2 = P(AXES, None)
    split_3 = P(AXES, None, None)
    return jax.shard_map(
        per_device,
        mesh=mesh,
        in_specs=(split_3,) + (split_2,) * 8 + (split_1, P(), split_1, split_2),
        out_specs=(split_2, split_3),
        check_vma=False,
    )
```

```python
import functools

import jax
import jax.numpy as jnp
from jax import lax
from jax.experimental import pallas as pl
from jax.experimental.pallas import tpu as pltpu
from jax.sharding import PartitionSpec as P

AXES = ("clump", "grp")
ORDER = ("grp", "clump")
LANES = 128
PIECE = 256
F32, BF16, I32 = jnp.float32, jnp.bfloat16, jnp.int32


def iota(shape, dim):
    return lax.broadcasted_iota(I32, shape, dim)


def split(x):
    high = x.astype(BF16)
    return high, (x - high.astype(F32)).astype(BF16)


def onehot(mask):
    return jnp.where(mask, 1.0, 0.0).astype(BF16)


def dot_nn(a, b):
    return lax.dot_general(a, b, (((1,), (0,)), ((), ())), preferred_element_type=F32)


def dot_nt(a, b):
    return lax.dot_general(a, b, (((1,), (1,)), ((), ())), preferred_element_type=F32)


def lookup(table, index):
    shape = index.shape
    lane, row = index & (LANES - 1), index >> 7
    out = None
    for r in range(table.shape[0]):
        line = jnp.broadcast_to(table[r : r + 1, :], shape)
        got = jnp.take_along_axis(line, lane, axis=1, mode="promise_in_bounds")
        out = got if out is None else jnp.where(row == r, got, out)
    return out


def as_row(x):
    return jnp.concatenate([x[s : s + 1, :] for s in range(x.shape[0])], axis=1)


def order_kernel(before):
    before[...] = onehot(iota(before.shape, 0) < iota(before.shape, 1))


def spread(hots, values):
    high, low = split(values)
    empty = jnp.zeros_like(high)
    count = len(hots)
    rows = [
        jnp.concatenate([empty, empty] * g + [high, low] + [empty, empty] * (count - 1 - g), axis=1)
        for g in range(count)
    ]
    lines = jnp.concatenate([h for hot in hots for h in (hot, hot)], axis=1)
    return dot_nt(lines, jnp.concatenate(rows, axis=0))


def unpack(got, n_dev, lines, stride, nv):
    rows = [got[pl.ds(k, n_dev, stride=stride), :] for k in range(lines)]
    flat = jnp.concatenate(rows, axis=0).T
    groups = [flat[g * nv : (g + 1) * nv] for g in range(LANES // nv)]
    return jnp.concatenate(split(jnp.concatenate(groups, axis=1)), axis=0)


def prepare_kernel(
    n_clump,
    n_group,
    cap,
    pcol,
    clu,
    lgrid,
    pwt,
    cwt,
    lwt,
    count,
    target,
    pft,
    scale,
    frac,
    before,
    live_scale,
    sum_scale,
    home_hot,
    weights,
    slot_hot,
    ids,
    slot_out,
    frac_out,
):
    frac_out[...] = frac[...]
    n_dev = n_clump * n_group
    cells, patches = home_hot.shape
    nv = live_scale.shape[0]
    groups = LANES // nv
    lines = cap // groups

    index = pcol[...]
    land = lookup(clu[...], index)
    home = lookup(lgrid[...], land)
    weight = pwt[...] * lookup(cwt[...], index) * lookup(lwt[...], land)
    position = iota(index.shape, 0) * LANES + iota(index.shape, 1)
    alive = position < count[...]

    goal = target[...]
    owner = goal // cells
    seat = owner % n_group * n_clump + owner // n_group
    owned = iota((n_dev, cells), 0) == seat
    rank = jnp.sum(jnp.where(owned, dot_nn(onehot(owned), before[...]), 0.0), axis=0, keepdims=True)
    rank = rank.astype(I32)
    slot = (rank % groups * lines + rank // groups) * n_dev + seat
    local = (goal - owner * cells + 1).astype(F32)
    named = jnp.where(owned, local, 0.0).astype(BF16)
    ids[...] = dot_nt(named, onehot(iota((LANES, cells), 0) == rank)) - 1.0
    slot_hot[...] = onehot(iota(slot_hot.shape, 0) == slot)
    slot_out[...] = jnp.where(alive, lookup(slot, home), -1)

    types = scale.shape[0]
    type_hot = onehot(iota((types, patches), 0) == as_row(pft[...]))
    scale_t = jnp.concatenate(split(scale[...]), axis=1).T
    factor = dot_nn(scale_t, type_hot)
    factor = factor[:nv] + factor[nv:]
    home_row = as_row(jnp.where(alive, home, -1))
    weight_row = as_row(jnp.where(alive, weight, 0.0))
    live_scale[...] = jnp.where(home_row >= 0, factor, 0.0)
    sum_scale[...] = factor * weight_row
    home_hot[...] = onehot(iota((cells, patches), 0) == home_row)
    w_high, w_low = split(jnp.broadcast_to(weight_row, weights.shape))
    weights[...] = jnp.where(iota(weights.shape, 0) == 0, w_high, w_low)


def local_kernel(
    n_dev, flux, live_scale, sum_scale, home_hot, weights, slot_hot, ids, send, kept
):
    nv = flux.shape[0]
    groups = LANES // nv
    part = slot_hot.shape[0] // groups
    lines = part // n_dev
    values = flux[...]
    high, low = split(values * sum_scale[...])
    sums = dot_nt(jnp.concatenate([high, low, weights[...]], axis=0), home_hot[...])
    kept[...] = values * live_scale[...]
    send[pl.ds(lines, n_dev, stride=lines + 1), :] = ids[...]
    den = sums[2 * nv : 2 * nv + 1] + sums[2 * nv + 1 : 2 * nv + 2]
    mean = (sums[:nv] + sums[nv : 2 * nv]) / jnp.maximum(den, 1.0)
    out = spread([slot_hot[g * part : (g + 1) * part, :] for g in range(groups)], mean)
    for k in range(lines):
        send[pl.ds(k, n_dev, stride=lines + 1), :] = out[k * n_dev : (k + 1) * n_dev, :]


def owner_kernel(n_dev, cap, got, frac, field, send, hot_out):
    nv, cells = field.shape
    groups = LANES // nv
    lines = cap // groups
    ids = got[pl.ds(lines, n_dev, stride=lines + 1), :]
    lane = iota((n_dev, cells), 1).astype(F32)
    hots = []
    for g in range(groups):
        named = [ids[:, k * groups + g : k * groups + g + 1] for k in range(lines)]
        hots.append(jnp.concatenate([onehot(lane == column) for column in named], axis=0))
    part = frac[...]
    rest = (1.0 - part) * field[...]
    own = spread(hots, jnp.broadcast_to(part, (nv, cells)))
    other = spread(hots, rest)
    for k in range(lines):
        at = slice(k * n_dev, (k + 1) * n_dev)
        row = got[pl.ds(k, n_dev, stride=lines + 1), :]
        send[pl.ds(k, n_dev, stride=lines), :] = own[at, :] * row + other[at, :]
    hot_out[...] = jnp.concatenate(hots, axis=0)


def finish_kernel(
    n_dev, cap, got, slot, kept, heard, hot, frac, field, merged_out, anomaly_out, buffer, merged, sem
):
    nv, patches = kept.shape
    pieces = buffer.shape[1] // PIECE
    copies = []
    lines = cap * nv // LANES
    replies = unpack(got, n_dev, lines, lines, nv)
    row = as_row(slot[...])
    for c in range(pieces):
        at = slice(c * PIECE, (c + 1) * PIECE)
        patch_hot = onehot(iota((n_dev * cap, PIECE), 0) == row[:, at])
        picked = dot_nn(replies, patch_hot)
        buffer[:, at] = kept[:, at] - (picked[:nv] + picked[nv:])
        copies.append(pltpu.make_async_copy(buffer.at[:, at], anomaly_out.at[:, at], sem.at[c]))
        copies[-1].start()
    placed = dot_nn(unpack(heard, n_dev, lines, lines + 1, nv), hot[...])
    part = frac[...]
    merged[...] = part * (placed[:nv] + placed[nv:]) + (1.0 - part) * field[...]
    copies.append(pltpu.make_async_copy(merged, merged_out, sem.at[pieces]))
    copies[-1].start()
    for copy in copies:
        copy.wait()


def shape(dims, dtype=F32):
    return jax.ShapeDtypeStruct(dims, dtype)


VMEM = pl.BlockSpec(memory_space=pltpu.VMEM)
HBM = pl.BlockSpec(memory_space=pltpu.HBM)


def call(body, outs, in_specs, flops, scratch=(), space=None):
    return pl.pallas_call(
        body,
        out_shape=outs,
        in_specs=in_specs,
        out_specs=[space or VMEM] * len(outs),
        scratch_shapes=list(scratch),
        compiler_params=pltpu.CompilerParams(vmem_limit_bytes=16 << 20),
        cost_estimate=pl.CostEstimate(flops=flops, bytes_accessed=1 << 20, transcendentals=0),
    )


def per_device(
    flux,
    patch_pft,
    patch_wt,
    patch_col,
    col_wt,
    col_lu,
    lu_wt,
    lu_grid,
    cell_target,
    patch_count,
    pft_scale,
    cpl_frac,
    cpl_field,
):
    n_clump, n_group = lax.axis_size("clump"), lax.axis_size("grp")
    n_dev = n_clump * n_group
    patches, nv = flux.shape[1:]
    cells = cell_target.shape[1]
    cap = max(2, 2 * cells // n_dev)
    lines = cap * nv // LANES
    lanes = lambda x: x.reshape(-1, LANES)

    def exchange(x):
        rows = x.shape[0] // n_dev
        whole = rows & (rows - 1) == 0
        x = x.reshape(n_dev, rows, LANES) if whole else x.reshape(n_dev, 1, rows * LANES)
        return lax.all_to_all(x, ORDER, split_axis=0, concat_axis=0, tiled=True).reshape(-1, LANES)

    (before,) = call(order_kernel, [shape((cells, cells), BF16)], [], 1 << 29)()
    *plan, slot, frac = call(
        functools.partial(prepare_kernel, n_clump, n_group, cap),
        [
            shape((nv, patches)),
            shape((nv, patches)),
            shape((cells, patches), BF16),
            shape((16, patches), BF16),
            shape((n_dev * cap, cells), BF16),
            shape((n_dev, LANES)),
            shape((patches // LANES, LANES), I32),
            shape((1, cells)),
        ],
        [VMEM] * 12,
        1 << 26,
    )(
        lanes(patch_col),
        lanes(col_lu),
        lanes(lu_grid),
        lanes(patch_wt),
        lanes(col_wt),
        lanes(lu_wt),
        patch_count.reshape(1, 1),
        cell_target,
        lanes(patch_pft),
        pft_scale,
        cpl_frac.reshape(1, cells),
        before,
    )
    send, kept = call(
        functools.partial(local_kernel, n_dev),
        [shape((n_dev * (lines + 1), LANES)), shape((nv, patches))],
        [VMEM] * 7,
        1 << 26,
    )(flux[0].T, *plan)
    field_t = cpl_field.T
    heard = exchange(send)
    reply, hot = call(
        functools.partial(owner_kernel, n_dev, cap),
        [shape((n_dev * lines, LANES)), shape((n_dev * cap, cells), BF16)],
        [VMEM] * 3,
        1 << 26,
    )(heard, frac, field_t)
    merged, anomaly = call(
        functools.partial(finish_kernel, n_dev, cap),
        [shape((nv, cells)), shape((nv, patches))],
        [VMEM] * 7,
        1 << 26,
        [
            pltpu.VMEM((nv, patches), F32),
            pltpu.VMEM((nv, cells), F32),
            pltpu.SemaphoreType.DMA((patches // PIECE + 1,)),
        ],
        HBM,
    )(exchange(reply), slot, kept, heard, hot, frac, field_t)
    return merged.T, anomaly.T[None]


def solution(mesh):
    split_1 = P(AXES)
    split_2 = P(AXES, None)
    split_3 = P(AXES, None, None)
    return jax.shard_map(
        per_device,
        mesh=mesh,
        in_specs=(split_3,) + (split_2,) * 8 + (split_1, P(), split_1, split_2),
        out_specs=(split_2, split_3),
        check_vma=False,
    )
```
